32 devices in a mesh: row: 8 (over z, y), col: 4 (over x, core).
Axes of the slice: x: 2, y: 2, z: 4, core: 2. Of those that a mesh axis runs over, the one named last changes fastest.
Arguments:
- embeddings: bfloat16 [5, 192, 2048], P(None, None, ('row', 'col')), may hold values from -6 to 6
- scale_weights: float32 [5], replicated, may hold values from 0.1 to 0.5
- vectors: bfloat16 [32, 2048], P(None, ('row', 'col')), may hold values from -6 to 6
Outputs:
- product: float32 [32, 2048], P(None, ('row', 'col'))
The draws below stay inside these ranges and needn't reach their ends.
All inputs are finite; a program needn't handle non-finite values.
Results may differ from the reference program's by a relative error of at most 0.011.
Values may be sent and summed in bfloat16 or wider, within the bound.
A program may use at most 64 MiB of HBM per device.

```python
import math
import jax
import jax.numpy as jnp
from jax import lax

DIM = 192
SCALES = 5
VECS = 32
SEGMENTS = 2048


def block_scale(stream_key, extent, cuts, least, top_value):
    loudness, own = 1.0, jax.random.fold_in(stream_key, 6)
    for position, parts in cuts:
        heights = jnp.exp(jax.random.uniform(jax.random.fold_in(own, position), (parts,), jnp.float32, least / len(cuts), top_value / len(cuts)))
        loudness = loudness * jnp.repeat(heights, extent[position] // parts).reshape([-1 if axis == position else 1 for axis in range(len(extent))])
    return loudness


def bell_draw(stream_key, extent, width, bound, split=(), kind=jnp.bfloat16):
    values = jax.random.normal(stream_key, extent, jnp.float32) * width
    if len(split) > 0:
        values = block_scale(stream_key, extent, split, -0.22, 0.18) * values
    return jnp.clip(values, min=-bound, max=bound).astype(kind)


def setup_inputs(seed: int = 0) -> dict:
    arg_keys = jax.random.split(jax.random.key(seed), 4)
    return {
        "embeddings": bell_draw(arg_keys[0], (SCALES, DIM, SEGMENTS), 1.0, 6.0, ((2, 32),)),
        "scale_weights": jnp.clip(jnp.exp(jax.random.uniform(arg_keys[1], (SCALES,), jnp.float32, math.log(0.1), math.log(0.5))), 0.1, 0.5),
        "vectors": bell_draw(arg_keys[2], (VECS, SEGMENTS), 1.0, 6.0, ((1, 32),)),
    }


SHARP = 3.5

def reference(embeddings, scale_weights, vectors):
    total = embeddings.shape[2]
    values = embeddings.astype(jnp.float32)
    units = values * lax.rsqrt(lax.optimization_barrier(jnp.sum(values * values, axis=1, keepdims=True)) + 1e-06)
    unit = lax.optimization_barrier(units.astype(jnp.bfloat16))
    weighted = (scale_weights[:, None, None] * unit.astype(jnp.float32)).astype(jnp.bfloat16)
    row_panel = weighted.reshape(-1, total)
    column_panel = unit.reshape(-1, total)
    sharpness = SHARP * math.sqrt(DIM)
    stride = math.gcd(total, 512)
    columns = jnp.arange(total, dtype=jnp.int32)

    def one_block(offset):
        rows = lax.dynamic_slice_in_dim(row_panel, offset, stride, 1)
        cosine = lax.dot_general(rows, column_panel, (((0,), (0,)), ((), ())), preferred_element_type=jnp.float32)
        row_ids = offset + jnp.arange(stride, dtype=jnp.int32)
        affinity = jnp.where(row_ids[:, None] == columns[None, :], jnp.zeros_like(cosine), jnp.exp(sharpness * cosine))
        degree = lax.optimization_barrier(jnp.sum(affinity, axis=1))
        numerator = lax.dot_general(vectors, affinity.astype(jnp.bfloat16), (((1,), (1,)), ((), ())), preferred_element_type=jnp.float32)
        return numerator / degree[None, :]
    offsets = jnp.arange(total // stride, dtype=jnp.int32) * stride
    blocks = lax.map(one_block, offsets)
    return jnp.transpose(blocks, (1, 0, 2)).reshape(vectors.shape[0], total)
```

```python
import functools
import math

import jax
import jax.numpy as jnp
from jax import lax
from jax.experimental import pallas as pl
from jax.experimental.pallas import tpu as pltpu
from jax.sharding import PartitionSpec as P

SHARP = 3.5
LANES = 128
CORES = 2
CHUNKS = 2
MESH = pl.DeviceIdType.MESH


def kernel(
    plan, emb_ref, scale_ref, vec_ref, out_ref, rows, cols, partial, landed,
    line_send, line_recv, own_send, own_recv, pair_send, pair_recv, part_send, part_recv,
):
    line, near, wide, width = plan
    scales, dim, segments = emb_ref.shape
    vecs = vec_ref.shape[0]
    feats = scales * dim
    row, col = lax.axis_index("row"), lax.axis_index("col")
    z, q = row // near, lax.rem(row, near)
    me = q * wide + col
    partner = col + 1 - 2 * lax.rem(col, CORES)

    def at(other_z, other_q, other_col):
        return (other_z * near + other_q, other_col)

    barrier = pltpu.get_barrier_semaphore()
    greeted = 0
    for step in (1, line - 1):
        if line > 1:
            pl.semaphore_signal(
                barrier, inc=1, device_id=at(lax.rem(z + step, line), q, col), device_id_type=MESH
            )
            greeted += 1
    for dq in range(near):
        for dc in range(wide):
            if dq or dc:
                pl.semaphore_signal(
                    barrier,
                    inc=1,
                    device_id=at(z, lax.rem(q + dq, near), lax.rem(col + dc, wide)),
                    device_id_type=MESH,
                )
                greeted += 1

    units, weights = [], []
    for s in range(scales):
        values = emb_ref[s].astype(jnp.float32)
        unit = values * lax.rsqrt(jnp.sum(values * values, axis=0, keepdims=True) + 1e-06)
        unit = unit.astype(jnp.bfloat16)
        units.append(unit)
        weights.append((scale_ref[s] * unit.astype(jnp.float32)).astype(jnp.bfloat16))
    rest = width - feats - vecs
    units += [vec_ref[...], jnp.ones((rest, segments), jnp.bfloat16)]
    weights.append(jnp.zeros((width - feats, segments), jnp.bfloat16))
    cols[z] = jnp.concatenate(units, axis=0).T
    rows[me] = jnp.concatenate(weights, axis=0).T
    pl.semaphore_wait(barrier, greeted)

    size = segments // CHUNKS

    def line_copy(up, step, chunk):
        block = z - step if up else z + step
        there = z + 1 if up else z - 1
        piece = cols.at[jnp.clip(block, 0, line - 1), pl.ds(chunk * size, size)]
        k = int(up)
        copy = pltpu.make_async_remote_copy(
            src_ref=piece,
            dst_ref=piece,
            send_sem=line_send.at[k, step, chunk],
            recv_sem=line_recv.at[k, step, chunk],
            device_id=at(jnp.clip(there, 0, line - 1), q, col),
            device_id_type=MESH,
        )
        sends = (z - step >= 0) & (z < line - 1) if up else (z + step <= line - 1) & (z > 0)
        return copy, sends

    def line_start(up, step, chunk):
        copy, sends = line_copy(up, step, chunk)
        pl.when(sends)(copy.start)

    def line_arrive(up, step, chunk):
        block = z - 1 - step if up else z + 1 + step
        piece = cols.at[jnp.clip(block, 0, line - 1), pl.ds(chunk * size, size)]
        gets = (z - 1 - step >= 0) if up else (z + 1 + step <= line - 1)

        @pl.when(gets)
        def _():
            pltpu.make_async_remote_copy(
                src_ref=piece,
                dst_ref=piece,
                send_sem=line_send.at[int(up), step, chunk],
                recv_sem=line_recv.at[int(up), step, chunk],
                device_id=at(jnp.clip(z - 1 if up else z + 1, 0, line - 1), q, col),
                device_id_type=MESH,
            ).wait_recv()

    hops = [(dq, dc) for dq in range(near) for dc in range(0, wide, CORES)]
    hops.sort(key=lambda hop: (hop[0] != 0) + (hop[1] != 0))

    def own_copy(k, slot, to):
        return pltpu.make_async_remote_copy(
            src_ref=rows.at[slot],
            dst_ref=rows.at[slot],
            send_sem=own_send.at[k],
            recv_sem=own_recv.at[k],
            device_id=to,
            device_id_type=MESH,
        )

    def source(k, column):
        dq, dc = hops[k]
        return lax.rem(q - dq + near, near) * wide + lax.rem(column - dc + wide, wide)

    def pair_copy(k, slot):
        return pltpu.make_async_remote_copy(
            src_ref=rows.at[slot],
            dst_ref=rows.at[slot],
            send_sem=pair_send.at[k],
            recv_sem=pair_recv.at[k],
            device_id=at(z, q, partner),
            device_id_type=MESH,
        )

    def hop_to(k):
        dq, dc = hops[k]
        return at(z, lax.rem(q + dq, near), lax.rem(col + dc, wide))

    for chunk in range(CHUNKS):
        for up in (True, False):
            if line > 1:
                line_start(up, 0, chunk)
    for k in range(1, len(hops)):
        own_copy(k, me, hop_to(k)).start()
    pair_copy(0, me).start()

    def plane_pass(k):
        slot = source(k, col)
        own_copy(k, slot, hop_to(k)).wait_recv()
        pair_copy(k, slot).start()

    todo = list(range(1, len(hops)))
    each = -(-len(todo) // max(line - 1, 1))
    for step in range(line - 1):
        for chunk in range(CHUNKS):
            for up in (True, False):
                line_arrive(up, step, chunk)
                if step + 1 < line - 1:
                    line_start(up, step + 1, chunk)
        for k in todo[step * each : (step + 1) * each]:
            plane_pass(k)
    for k in todo[(line - 1) * each :]:
        plane_pass(k)
    for k in range(len(hops)):
        pair_copy(k, source(k, partner)).wait_recv()

    sharpness = SHARP * math.sqrt(dim)
    count = line * segments
    columns = cols[...].reshape(count, width)
    base = feats // LANES * LANES
    tail = columns[:, base:]
    positions = lax.broadcasted_iota(jnp.int32, (1, count), 1)
    column_ids = (positions // segments * (near * wide) + me) * segments + positions % segments
    for step in range(1, near + 1):
        other = lax.rem(q + step, near)
        first = other * wide
        panel = rows[pl.ds(first, wide)].reshape(wide * segments, width)
        cosine = lax.dot_general(
            panel, columns, (((1,), (1,)), ((), ())), preferred_element_type=jnp.float32
        )
        row_ids = (z * near * wide + first) * segments + lax.broadcasted_iota(
            jnp.int32, (wide * segments, 1), 0
        )
        affinity = jnp.where(
            row_ids == column_ids, jnp.zeros_like(cosine), jnp.exp(sharpness * cosine)
        )
        sums = lax.dot_general(
            affinity.astype(jnp.bfloat16), tail, (((1,), (0,)), ((), ())),
            preferred_element_type=jnp.float32,
        )
        partial[pl.ds(first, wide)] = sums.reshape(wide, segments, width - base)

        for dc in range(wide):
            dq = step % near
            if dq or dc:
                k = dq * wide + dc
                to = lax.rem(col + dc, wide)
                pltpu.make_async_remote_copy(
                    src_ref=partial.at[first + to],
                    dst_ref=landed.at[k],
                    send_sem=part_send.at[k],
                    recv_sem=part_recv.at[k],
                    device_id=at(z, other, to),
                    device_id_type=MESH,
                ).start()

    def part_copy(k):
        dq, dc = k // wide, k % wide
        other, to = lax.rem(q + dq, near), lax.rem(col + dc, wide)
        return pltpu.make_async_remote_copy(
            src_ref=partial.at[other * wide + to],
            dst_ref=landed.at[k],
            send_sem=part_send.at[k],
            recv_sem=part_recv.at[k],
            device_id=at(z, other, to),
            device_id_type=MESH,
        )

    total = partial[me]
    for k in range(1, near * wide):
        part_copy(k).wait_recv()
        total = total + landed[k]
    total = total.T
    low = feats - base
    out_ref[...] = total[low : low + vecs] / total[low + vecs : low + vecs + 1]

    for k in range(1, near * wide):
        part_copy(k).wait_send()
    for k in range(len(hops)):
        if k:
            own_copy(k, me, hop_to(k)).wait_send()
        pair_copy(k, source(k, col)).wait_send()
    for step in range(line - 1):
        for chunk in range(CHUNKS):
            for up in (True, False):
                copy, sends = line_copy(up, step, chunk)
                pl.when(sends)(copy.wait_send)


def shards(shape, embeddings, scale_weights, vectors):
    row_count, wide = shape
    near = math.gcd(row_count, 2)
    line = row_count // near
    scales, dim, segments = embeddings.shape
    vecs = vectors.shape[0]
    feats = scales * dim
    width = -(-(feats + vecs + 1) // LANES) * LANES
    plane = near * wide
    base = feats // LANES * LANES
    hops = near * wide // CORES
    steps = max(line - 1, 1)
    dma = pltpu.SemaphoreType.DMA
    return pl.pallas_call(
        functools.partial(kernel, (line, near, wide, width)),
        out_shape=jax.ShapeDtypeStruct((vecs, segments), jnp.float32),
        in_specs=[
            pl.BlockSpec(memory_space=pltpu.VMEM),
            pl.BlockSpec(memory_space=pltpu.SMEM),
            pl.BlockSpec(memory_space=pltpu.VMEM),
        ],
        out_specs=pl.BlockSpec(memory_space=pltpu.VMEM),
        scratch_shapes=[
            pltpu.VMEM((plane, segments, width), jnp.bfloat16),
            pltpu.VMEM((line, segments, width), jnp.bfloat16),
            pltpu.VMEM((plane, segments, width - base), jnp.float32),
            pltpu.VMEM((plane, segments, width - base), jnp.float32),
            dma((2, steps, CHUNKS)),
            dma((2, steps, CHUNKS)),
            dma((hops,)),
            dma((hops,)),
            dma((hops,)),
            dma((hops,)),
            dma((plane,)),
            dma((plane,)),
        ],
        compiler_params=pltpu.CompilerParams(
            collective_id=0, has_side_effects=True, vmem_limit_bytes=56 * 1024 * 1024
        ),
    )(embeddings, scale_weights, vectors)


def solution(mesh):
    placed = (P(None, None, ("row", "col")), P(), P(None, ("row", "col")))
    return jax.shard_map(
        functools.partial(shards, (mesh.shape["row"], mesh.shape["col"])),
        mesh=mesh, in_specs=placed, out_specs=P(None, ("row", "col")), check_vma=False,
    )
```

```python
import functools
import math

import jax
import jax.numpy as jnp
from jax import lax
from jax.experimental import pallas as pl
from jax.experimental.pallas import tpu as pltpu
from jax.sharding import PartitionSpec as P

SHARP = 3.5
LANES = 128
CORES = 2
CHUNKS = 2
MESH = pl.DeviceIdType.MESH


def kernel(
    plan, emb_ref, scale_ref, vec_ref, out_ref, rows, cols, partial, landed,
    line_send, line_recv, own_send, own_recv, pair_send, pair_recv, part_send, part_recv,
):
    line, near, wide, width = plan
    scales, segments, dim = emb_ref.shape
    vecs = vec_ref.shape[0]
    feats = scales * dim
    row, col = lax.axis_index("row"), lax.axis_index("col")
    z, q = row // near, lax.rem(row, near)
    me = q * wide + col
    partner = col + 1 - 2 * lax.rem(col, CORES)

    def at(other_z, other_q, other_col):
        return (other_z * near + other_q, other_col)

    barrier = pltpu.get_barrier_semaphore()
    greeted = 0
    for step in (1, line - 1):
        if line > 1:
            pl.semaphore_signal(
                barrier, inc=1, device_id=at(lax.rem(z + step, line), q, col), device_id_type=MESH
            )
            greeted += 1
    for dq in range(near):
        for dc in range(wide):
            if dq or dc:
                pl.semaphore_signal(
                    barrier,
                    inc=1,
                    device_id=at(z, lax.rem(q + dq, near), lax.rem(col + dc, wide)),
                    device_id_type=MESH,
                )
                greeted += 1

    whole = dim // LANES * LANES
    units, unit_rests, weights, weight_rests = [], [], [], []
    for s in range(scales):
        values = emb_ref[s].astype(jnp.float32)
        unit = values * lax.rsqrt(jnp.sum(values * values, axis=1, keepdims=True) + 1e-06)
        unit = unit.astype(jnp.bfloat16)
        weighted = (scale_ref[s] * unit.astype(jnp.float32)).astype(jnp.bfloat16)
        units.append(unit[:, :whole])
        unit_rests.append(unit[:, whole:])
        weights.append(weighted[:, :whole])
        weight_rests.append(weighted[:, whole:])
    ones = jnp.ones((segments, width - feats - vecs), jnp.bfloat16)
    zeros = jnp.zeros((segments, width - feats), jnp.bfloat16)
    cols[z] = jnp.concatenate(units + unit_rests + [vec_ref[...].T, ones], axis=1)
    rows[me] = jnp.concatenate(weights + weight_rests + [zeros], axis=1)
    pl.semaphore_wait(barrier, greeted)

    size = segments // CHUNKS

    def line_copy(up, step, chunk):
        block = z - step if up else z + step
        there = z + 1 if up else z - 1
        piece = cols.at[jnp.clip(block, 0, line - 1), pl.ds(chunk * size, size)]
        k = int(up)
        copy = pltpu.make_async_remote_copy(
            src_ref=piece,
            dst_ref=piece,
            send_sem=line_send.at[k, step, chunk],
            recv_sem=line_recv.at[k, step, chunk],
            device_id=at(jnp.clip(there, 0, line - 1), q, col),
            device_id_type=MESH,
        )
        sends = (z - step >= 0) & (z < line - 1) if up else (z + step <= line - 1) & (z > 0)
        return copy, sends

    def line_start(up, step, chunk):
        copy, sends = line_copy(up, step, chunk)
        pl.when(sends)(copy.start)

    def line_arrive(up, step, chunk):
        block = z - 1 - step if up else z + 1 + step
        piece = cols.at[jnp.clip(block, 0, line - 1), pl.ds(chunk * size, size)]
        gets = (z - 1 - step >= 0) if up else (z + 1 + step <= line - 1)

        @pl.when(gets)
        def _():
            pltpu.make_async_remote_copy(
                src_ref=piece,
                dst_ref=piece,
                send_sem=line_send.at[int(up), step, chunk],
                recv_sem=line_recv.at[int(up), step, chunk],
                device_id=at(jnp.clip(z - 1 if up else z + 1, 0, line - 1), q, col),
                device_id_type=MESH,
            ).wait_recv()

    hops = [(dq, dc) for dq in range(near) for dc in range(0, wide, CORES)]
    hops.sort(key=lambda hop: (hop[0] != 0) + (hop[1] != 0))

    def own_copy(k, slot, to):
        return pltpu.make_async_remote_copy(
            src_ref=rows.at[slot],
            dst_ref=rows.at[slot],
            send_sem=own_send.at[k],
            recv_sem=own_recv.at[k],
            device_id=to,
            device_id_type=MESH,
        )

    def source(k, column):
        dq, dc = hops[k]
        return lax.rem(q - dq + near, near) * wide + lax.rem(column - dc + wide, wide)

    def pair_copy(k, slot):
        return pltpu.make_async_remote_copy(
            src_ref=rows.at[slot],
            dst_ref=rows.at[slot],
            send_sem=pair_send.at[k],
            recv_sem=pair_recv.at[k],
            device_id=at(z, q, partner),
            device_id_type=MESH,
        )

    def hop_to(k):
        dq, dc = hops[k]
        return at(z, lax.rem(q + dq, near), lax.rem(col + dc, wide))

    for chunk in range(CHUNKS):
        for up in (True, False):
            if line > 1:
                line_start(up, 0, chunk)
    for k in range(1, len(hops)):
        own_copy(k, me, hop_to(k)).start()
    pair_copy(0, me).start()

    def plane_pass(k):
        slot = source(k, col)
        own_copy(k, slot, hop_to(k)).wait_recv()
        pair_copy(k, slot).start()

    todo = list(range(1, len(hops)))
    each = -(-len(todo) // max(line - 1, 1))
    for step in range(line - 1):
        for chunk in range(CHUNKS):
            for up in (True, False):
                line_arrive(up, step, chunk)
                if step + 1 < line - 1:
                    line_start(up, step + 1, chunk)
        for k in todo[step * each : (step + 1) * each]:
            plane_pass(k)
    for k in todo[(line - 1) * each :]:
        plane_pass(k)
    for k in range(len(hops)):
        pair_copy(k, source(k, partner)).wait_recv()

    sharpness = SHARP * math.sqrt(dim)
    count = line * segments
    columns = cols[...].reshape(count, width)
    base = feats // LANES * LANES
    tail = columns[:, base:]
    positions = lax.broadcasted_iota(jnp.int32, (1, count), 1)
    column_ids = (positions // segments * (near * wide) + me) * segments + positions % segments
    for step in range(1, near + 1):
        other = lax.rem(q + step, near)
        first = other * wide
        panel = rows[pl.ds(first, wide)].reshape(wide * segments, width)
        cosine = lax.dot_general(
            panel, columns, (((1,), (1,)), ((), ())), preferred_element_type=jnp.float32
        )
        row_ids = (z * near * wide + first) * segments + lax.broadcasted_iota(
            jnp.int32, (wide * segments, 1), 0
        )
        affinity = jnp.where(
            row_ids == column_ids, jnp.zeros_like(cosine), jnp.exp(sharpness * cosine)
        )
        sums = lax.dot_general(
            affinity.astype(jnp.bfloat16), tail, (((1,), (0,)), ((), ())),
            preferred_element_type=jnp.float32,
        )
        partial[pl.ds(first, wide)] = sums.reshape(wide, segments, width - base)

        for dc in range(wide):
            dq = step % near
            if dq or dc:
                k = dq * wide + dc
                to = lax.rem(col + dc, wide)
                pltpu.make_async_remote_copy(
                    src_ref=partial.at[first + to],
                    dst_ref=landed.at[k],
                    send_sem=part_send.at[k],
                    recv_sem=part_recv.at[k],
                    device_id=at(z, other, to),
                    device_id_type=MESH,
                ).start()

    def part_copy(k):
        dq, dc = k // wide, k % wide
        other, to = lax.rem(q + dq, near), lax.rem(col + dc, wide)
        return pltpu.make_async_remote_copy(
            src_ref=partial.at[other * wide + to],
            dst_ref=landed.at[k],
            send_sem=part_send.at[k],
            recv_sem=part_recv.at[k],
            device_id=at(z, other, to),
            device_id_type=MESH,
        )

    total = partial[me]
    for k in range(1, near * wide):
        part_copy(k).wait_recv()
        total = total + landed[k]
    total = total.T
    low = feats - base
    out_ref[...] = total[low : low + vecs] / total[low + vecs : low + vecs + 1]

    for k in range(1, near * wide):
        part_copy(k).wait_send()
    for k in range(len(hops)):
        if k:
            own_copy(k, me, hop_to(k)).wait_send()
        pair_copy(k, source(k, col)).wait_send()
    for step in range(line - 1):
        for chunk in range(CHUNKS):
            for up in (True, False):
                copy, sends = line_copy(up, step, chunk)
                pl.when(sends)(copy.wait_send)


def shards(shape, embeddings, scale_weights, vectors):
    row_count, wide = shape
    near = math.gcd(row_count, 2)
    line = row_count // near
    scales, dim, segments = embeddings.shape
    vecs = vectors.shape[0]
    feats = scales * dim
    width = -(-(feats + vecs + 1) // LANES) * LANES
    plane = near * wide
    base = feats // LANES * LANES
    hops = near * wide // CORES
    steps = max(line - 1, 1)
    dma = pltpu.SemaphoreType.DMA
    return pl.pallas_call(
        functools.partial(kernel, (line, near, wide, width)),
        out_shape=jax.ShapeDtypeStruct((vecs, segments), jnp.float32),
        in_specs=[
            pl.BlockSpec(memory_space=pltpu.VMEM),
            pl.BlockSpec(memory_space=pltpu.SMEM),
            pl.BlockSpec(memory_space=pltpu.VMEM),
        ],
        out_specs=pl.BlockSpec(memory_space=pltpu.VMEM),
        scratch_shapes=[
            pltpu.VMEM((plane, segments, width), jnp.bfloat16),
            pltpu.VMEM((line, segments, width), jnp.bfloat16),
            pltpu.VMEM((plane, segments, width - base), jnp.float32),
            pltpu.VMEM((plane, segments, width - base), jnp.float32),
            dma((2, steps, CHUNKS)),
            dma((2, steps, CHUNKS)),
            dma((hops,)),
            dma((hops,)),
            dma((hops,)),
            dma((hops,)),
            dma((plane,)),
            dma((plane,)),
        ],
        compiler_params=pltpu.CompilerParams(
            collective_id=0, has_side_effects=True, vmem_limit_bytes=56 * 1024 * 1024
        ),
    )(jnp.swapaxes(embeddings, 1, 2), scale_weights, vectors)


def solution(mesh):
    placed = (P(None, None, ("row", "col")), P(), P(None, ("row", "col")))
    return jax.shard_map(
        functools.partial(shards, (mesh.shape["row"], mesh.shape["col"])),
        mesh=mesh, in_specs=placed, out_specs=P(None, ("row", "col")), check_vma=False,
    )
```

```python
import functools
import math

import jax
import jax.numpy as jnp
from jax import lax
from jax.experimental import pallas as pl
from jax.experimental.pallas import tpu as pltpu
from jax.sharding import PartitionSpec as P

SHARP = 3.5
LANES = 128
CORES = 2
CHUNKS = 4
MESH = pl.DeviceIdType.MESH


def kernel(
    plan, emb_ref, scale_ref, vec_ref, out_ref, values_ref, load_sem, rows, cols, partial, landed,
    line_send, line_recv, own_send, own_recv, pair_send, pair_recv, part_send, part_recv,
):
    line, near, wide, width = plan
    scales, segments, dim = emb_ref.shape
    vecs = vec_ref.shape[0]
    feats = scales * dim
    row, col = lax.axis_index("row"), lax.axis_index("col")
    z, q = row // near, lax.rem(row, near)
    me = q * wide + col
    partner = col + 1 - 2 * lax.rem(col, CORES)

    def at(other_z, other_q, other_col):
        return (other_z * near + other_q, other_col)

    load = pltpu.make_async_copy(emb_ref, values_ref, load_sem)
    load.start()
    barrier = pltpu.get_barrier_semaphore()
    greeted = (z > 0).astype(jnp.int32) + (z < line - 1).astype(jnp.int32)

    def greet(device):
        pl.semaphore_signal(barrier, inc=1, device_id=device, device_id_type=MESH)

    pl.when(z > 0)(lambda: greet(at(z - 1, q, col)))
    pl.when(z < line - 1)(lambda: greet(at(z + 1, q, col)))
    greet(at(z, q, partner))
    greeted = greeted + 1
    for dc in range(CORES, wide, CORES):
        greet(at(z, q, lax.rem(col + dc, wide)))
        greeted = greeted + 1
    if near > 1:
        greet(at(z, 1 - q, col))
        greeted = greeted + 1
    load.wait()

    whole = dim // LANES * LANES
    units, unit_rests, weights, weight_rests = [], [], [], []
    for s in range(scales):
        values = values_ref[s].astype(jnp.float32)
        unit = values * lax.rsqrt(jnp.sum(values * values, axis=1, keepdims=True) + 1e-06)
        unit = unit.astype(jnp.bfloat16)
        weighted = (scale_ref[s] * unit.astype(jnp.float32)).astype(jnp.bfloat16)
        units.append(unit[:, :whole])
        unit_rests.append(unit[:, whole:])
        weights.append(weighted[:, :whole])
        weight_rests.append(weighted[:, whole:])
    ones = jnp.ones((segments, width - feats - vecs), jnp.bfloat16)
    zeros = jnp.zeros((segments, width - feats), jnp.bfloat16)
    cols[z] = jnp.concatenate(units + unit_rests + [vec_ref[...].T, ones], axis=1)
    rows[me] = jnp.concatenate(weights + weight_rests + [zeros], axis=1)
    pl.semaphore_wait(barrier, greeted)

    size = segments // CHUNKS

    def line_copy(up, step, chunk):
        block = z - step if up else z + step
        there = z + 1 if up else z - 1
        piece = cols.at[jnp.clip(block, 0, line - 1), pl.ds(chunk * size, size)]
        k = int(up)
        copy = pltpu.make_async_remote_copy(
            src_ref=piece,
            dst_ref=piece,
            send_sem=line_send.at[k, step, chunk],
            recv_sem=line_recv.at[k, step, chunk],
            device_id=at(jnp.clip(there, 0, line - 1), q, col),
            device_id_type=MESH,
        )
        sends = (z - step >= 0) & (z < line - 1) if up else (z + step <= line - 1) & (z > 0)
        return copy, sends

    def line_start(up, step, chunk):
        copy, sends = line_copy(up, step, chunk)
        pl.when(sends)(copy.start)

    def line_arrive(up, step, chunk):
        block = z - 1 - step if up else z + 1 + step
        piece = cols.at[jnp.clip(block, 0, line - 1), pl.ds(chunk * size, size)]
        gets = (z - 1 - step >= 0) if up else (z + 1 + step <= line - 1)

        @pl.when(gets)
        def _():
            pltpu.make_async_remote_copy(
                src_ref=piece,
                dst_ref=piece,
                send_sem=line_send.at[int(up), step, chunk],
                recv_sem=line_recv.at[int(up), step, chunk],
                device_id=at(jnp.clip(z - 1 if up else z + 1, 0, line - 1), q, col),
                device_id_type=MESH,
            ).wait_recv()

    hops = [(dq, dc) for dq in range(near) for dc in range(0, wide, CORES)]
    pairs = wide // CORES

    def own_copy(k, slot, to):
        return pltpu.make_async_remote_copy(
            src_ref=rows.at[slot],
            dst_ref=rows.at[slot],
            send_sem=own_send.at[k],
            recv_sem=own_recv.at[k],
            device_id=to,
            device_id_type=MESH,
        )

    def source(k, column):
        dq, dc = hops[k]
        return lax.rem(q - dq + near, near) * wide + lax.rem(column - dc + wide, wide)

    def pair_copy(k, slot):
        return pltpu.make_async_remote_copy(
            src_ref=rows.at[slot],
            dst_ref=rows.at[slot],
            send_sem=pair_send.at[k],
            recv_sem=pair_recv.at[k],
            device_id=at(z, q, partner),
            device_id_type=MESH,
        )

    def hop_to(k):
        dq, dc = hops[k]
        return at(z, 1 - q, col) if dq else at(z, q, lax.rem(col + dc, wide))

    def relay(k):
        if near > 1:
            own_copy(k + pairs, source(k, col), hop_to(k + pairs)).start()

    for chunk in range(CHUNKS):
        for up in (True, False):
            if line > 1:
                line_start(up, 0, chunk)
    for k in range(1, pairs):
        own_copy(k, me, hop_to(k)).start()
    relay(0)
    pair_copy(0, me).start()

    def plane_pass(k):
        slot = source(k, col)
        own_copy(k, slot, hop_to(k)).wait_recv()
        if k < pairs:
            relay(k)
        pair_copy(k, slot).start()

    todo = list(range(1, len(hops)))
    each = -(-len(todo) // max(line - 1, 1))
    for step in range(line - 1):
        for chunk in range(CHUNKS):
            for up in (True, False):
                line_arrive(up, step, chunk)
                if step + 1 < line - 1:
                    line_start(up, step + 1, chunk)
        for k in todo[step * each : (step + 1) * each]:
            plane_pass(k)
    for k in todo[(line - 1) * each :]:
        plane_pass(k)
    for k in range(len(hops)):
        pair_copy(k, source(k, partner)).wait_recv()

    sharpness = SHARP * math.sqrt(dim)
    count = line * segments
    columns = cols[...].reshape(count, width)
    base = feats // LANES * LANES
    tail = columns[:, base:]
    positions = lax.broadcasted_iota(jnp.int32, (1, count), 1)
    column_ids = (positions // segments * (near * wide) + me) * segments + positions % segments
    for step in range(1, near + 1):
        other = lax.rem(q + step, near)
        first = other * wide
        panel = rows[pl.ds(first, wide)].reshape(wide * segments, width)
        cosine = lax.dot_general(
            panel, columns, (((1,), (1,)), ((), ())), preferred_element_type=jnp.float32
        )
        row_ids = (z * near * wide + first) * segments + lax.broadcasted_iota(
            jnp.int32, (wide * segments, 1), 0
        )
        affinity = jnp.where(
            row_ids == column_ids, jnp.zeros_like(cosine), jnp.exp(sharpness * cosine)
        )
        sums = lax.dot_general(
            affinity.astype(jnp.bfloat16), tail, (((1,), (0,)), ((), ())),
            preferred_element_type=jnp.float32,
        )
        partial[pl.ds(first, wide)] = sums.astype(jnp.bfloat16).reshape(wide, segments, width - base)

        for dc in range(wide):
            dq = step % near
            if dq or dc:
                k = dq * wide + dc
                to = lax.rem(col + dc, wide)
                pltpu.make_async_remote_copy(
                    src_ref=partial.at[first + to],
                    dst_ref=landed.at[k],
                    send_sem=part_send.at[k],
                    recv_sem=part_recv.at[k],
                    device_id=at(z, other, to),
                    device_id_type=MESH,
                ).start()

    def part_copy(k):
        dq, dc = k // wide, k % wide
        other, to = lax.rem(q + dq, near), lax.rem(col + dc, wide)
        return pltpu.make_async_remote_copy(
            src_ref=partial.at[other * wide + to],
            dst_ref=landed.at[k],
            send_sem=part_send.at[k],
            recv_sem=part_recv.at[k],
            device_id=at(z, other, to),
            device_id_type=MESH,
        )

    total = partial[me].astype(jnp.float32)
    for k in range(1, near * wide):
        part_copy(k).wait_recv()
        total = total + landed[k].astype(jnp.float32)
    total = total.T
    low = feats - base
    out_ref[...] = total[low : low + vecs] / total[low + vecs : low + vecs + 1]

    for k in range(1, near * wide):
        part_copy(k).wait_send()
    for k in range(len(hops)):
        if k:
            own_copy(k, me, hop_to(k)).wait_send()
        pair_copy(k, source(k, col)).wait_send()
    for step in range(line - 1):
        for chunk in range(CHUNKS):
            for up in (True, False):
                copy, sends = line_copy(up, step, chunk)
                pl.when(sends)(copy.wait_send)


def shards(shape, embeddings, scale_weights, vectors):
    row_count, wide = shape
    near = math.gcd(row_count, 2)
    line = row_count // near
    scales, dim, segments = embeddings.shape
    vecs = vectors.shape[0]
    feats = scales * dim
    width = -(-(feats + vecs + 1) // LANES) * LANES
    plane = near * wide
    base = feats // LANES * LANES
    hops = near * wide // CORES
    steps = max(line - 1, 1)
    dma = pltpu.SemaphoreType.DMA
    return pl.pallas_call(
        functools.partial(kernel, (line, near, wide, width)),
        out_shape=jax.ShapeDtypeStruct((vecs, segments), jnp.float32),
        in_specs=[
            pl.BlockSpec(memory_space=pl.ANY),
            pl.BlockSpec(memory_space=pltpu.SMEM),
            pl.BlockSpec(memory_space=pltpu.VMEM),
        ],
        out_specs=pl.BlockSpec(memory_space=pltpu.VMEM),
        scratch_shapes=[
            pltpu.VMEM((scales, segments, dim), jnp.bfloat16),
            dma,
            pltpu.VMEM((plane, segments, width), jnp.bfloat16),
            pltpu.VMEM((line, segments, width), jnp.bfloat16),
            pltpu.VMEM((plane, segments, width - base), jnp.bfloat16),
            pltpu.VMEM((plane, segments, width - base), jnp.bfloat16),
            dma((2, steps, CHUNKS)),
            dma((2, steps, CHUNKS)),
            dma((hops,)),
            dma((hops,)),
            dma((hops,)),
            dma((hops,)),
            dma((plane,)),
            dma((plane,)),
        ],
        compiler_params=pltpu.CompilerParams(
            collective_id=0, has_side_effects=True, vmem_limit_bytes=56 * 1024 * 1024
        ),
    )(jnp.swapaxes(embeddings, 1, 2), scale_weights, vectors)


def solution(mesh):
    placed = (P(None, None, ("row", "col")), P(), P(None, ("row", "col")))
    return jax.shard_map(
        functools.partial(shards, (mesh.shape["row"], mesh.shape["col"])),
        mesh=mesh, in_specs=placed, out_specs=P(None, ("row", "col")), check_vma=False,
    )
```

```python
import functools
import math

import jax
import jax.numpy as jnp
from jax import lax
from jax.experimental import pallas as pl
from jax.experimental.pallas import tpu as pltpu
from jax.sharding import PartitionSpec as P

SHARP = 3.5
LANES = 128
CORES = 2
CHUNKS = 4
PIECES = 2
MESH = pl.DeviceIdType.MESH


def kernel(
    plan, emb_ref, scale_ref, vec_ref, out_ref, values_ref, load_sem, rows, cols, partial, landed,
    line_send, line_recv, own_send, own_recv, pair_send, pair_recv, part_send, part_recv,
):
    line, near, wide, width = plan
    scales, segments, dim = emb_ref.shape
    vecs = vec_ref.shape[0]
    feats = scales * dim
    row, col = lax.axis_index("row"), lax.axis_index("col")
    z, q = row // near, lax.rem(row, near)
    me = q * wide + col
    partner = col + 1 - 2 * lax.rem(col, CORES)

    def at(other_z, other_q, other_col):
        return (other_z * near + other_q, other_col)

    load = pltpu.make_async_copy(emb_ref, values_ref, load_sem)
    load.start()
    barrier = pltpu.get_barrier_semaphore()
    greeted = (z > 0).astype(jnp.int32) + (z < line - 1).astype(jnp.int32)

    def greet(device):
        pl.semaphore_signal(barrier, inc=1, device_id=device, device_id_type=MESH)

    pl.when(z > 0)(lambda: greet(at(z - 1, q, col)))
    pl.when(z < line - 1)(lambda: greet(at(z + 1, q, col)))
    greet(at(z, q, partner))
    greeted = greeted + 1
    for dc in range(CORES, wide, CORES):
        greet(at(z, q, lax.rem(col + dc, wide)))
        greeted = greeted + 1
    if near > 1:
        greet(at(z, 1 - q, col))
        greeted = greeted + 1
    load.wait()

    whole = dim // LANES * LANES
    units, unit_rests, weights, weight_rests = [], [], [], []
    for s in range(scales):
        values = values_ref[s].astype(jnp.float32)
        unit = values * lax.rsqrt(jnp.sum(values * values, axis=1, keepdims=True) + 1e-06)
        unit = unit.astype(jnp.bfloat16)
        weighted = (scale_ref[s] * unit.astype(jnp.float32)).astype(jnp.bfloat16)
        units.append(unit[:, :whole])
        unit_rests.append(unit[:, whole:])
        weights.append(weighted[:, :whole])
        weight_rests.append(weighted[:, whole:])
    ones = jnp.ones((segments, width - feats - vecs), jnp.bfloat16)
    zeros = jnp.zeros((segments, width - feats), jnp.bfloat16)
    cols[z] = jnp.concatenate(units + unit_rests + [vec_ref[...].T, ones], axis=1)
    rows[me] = jnp.concatenate(weights + weight_rests + [zeros], axis=1)
    pl.semaphore_wait(barrier, greeted)

    size = segments // CHUNKS

    def line_copy(up, step, chunk):
        block = z - step if up else z + step
        there = z + 1 if up else z - 1
        piece = cols.at[jnp.clip(block, 0, line - 1), pl.ds(chunk * size, size)]
        k = int(up)
        copy = pltpu.make_async_remote_copy(
            src_ref=piece,
            dst_ref=piece,
            send_sem=line_send.at[k, step, chunk],
            recv_sem=line_recv.at[k, step, chunk],
            device_id=at(jnp.clip(there, 0, line - 1), q, col),
            device_id_type=MESH,
        )
        sends = (z - step >= 0) & (z < line - 1) if up else (z + step <= line - 1) & (z > 0)
        return copy, sends

    def line_start(up, step, chunk):
        copy, sends = line_copy(up, step, chunk)
        pl.when(sends)(copy.start)

    def line_arrive(up, step, chunk):
        block = z - 1 - step if up else z + 1 + step
        piece = cols.at[jnp.clip(block, 0, line - 1), pl.ds(chunk * size, size)]
        gets = (z - 1 - step >= 0) if up else (z + 1 + step <= line - 1)

        @pl.when(gets)
        def _():
            pltpu.make_async_remote_copy(
                src_ref=piece,
                dst_ref=piece,
                send_sem=line_send.at[int(up), step, chunk],
                recv_sem=line_recv.at[int(up), step, chunk],
                device_id=at(jnp.clip(z - 1 if up else z + 1, 0, line - 1), q, col),
                device_id_type=MESH,
            ).wait_recv()

    hops = [(dq, dc) for dq in range(near) for dc in range(0, wide, CORES)]
    pairs = wide // CORES

    part = segments // PIECES

    def own_copy(k, piece, slot, to):
        block = rows.at[slot, pl.ds(piece * part, part)]
        return pltpu.make_async_remote_copy(
            src_ref=block,
            dst_ref=block,
            send_sem=own_send.at[k, piece],
            recv_sem=own_recv.at[k, piece],
            device_id=to,
            device_id_type=MESH,
        )

    def source(k, column):
        dq, dc = hops[k]
        return lax.rem(q - dq + near, near) * wide + lax.rem(column - dc + wide, wide)

    def pair_copy(k, piece, slot):
        block = rows.at[slot, pl.ds(piece * part, part)]
        return pltpu.make_async_remote_copy(
            src_ref=block,
            dst_ref=block,
            send_sem=pair_send.at[k, piece],
            recv_sem=pair_recv.at[k, piece],
            device_id=at(z, q, partner),
            device_id_type=MESH,
        )

    def hop_to(k):
        dq, dc = hops[k]
        return at(z, 1 - q, col) if dq else at(z, q, lax.rem(col + dc, wide))

    def relay(k, piece):
        if near > 1:
            own_copy(k + pairs, piece, source(k, col), hop_to(k + pairs)).start()

    for chunk in range(CHUNKS):
        for up in (True, False):
            if line > 1:
                line_start(up, 0, chunk)
    for piece in range(PIECES):
        for k in range(1, pairs):
            own_copy(k, piece, me, hop_to(k)).start()
        relay(0, piece)
        pair_copy(0, piece, me).start()

    def plane_pass(k, piece):
        slot = source(k, col)
        own_copy(k, piece, slot, hop_to(k)).wait_recv()
        if k < pairs:
            relay(k, piece)
        pair_copy(k, piece, slot).start()

    todo = [(k, piece) for k in range(1, len(hops)) for piece in range(PIECES)]
    turns = (line - 1) * CHUNKS
    due = [1 + e * max(turns - CHUNKS + 1, 0) // max(len(todo), 1) for e in range(len(todo))]
    for turn in range(turns):
        step, chunk = turn // CHUNKS, turn % CHUNKS
        for up in (True, False):
            line_arrive(up, step, chunk)
            if step + 1 < line - 1:
                line_start(up, step + 1, chunk)
        for event, when in zip(todo, due):
            if when == turn:
                plane_pass(*event)
    for event, when in zip(todo, due):
        if when >= turns:
            plane_pass(*event)
    for k in range(len(hops)):
        for piece in range(PIECES):
            pair_copy(k, piece, source(k, partner)).wait_recv()

    sharpness = SHARP * math.sqrt(dim)
    count = line * segments
    columns = cols[...].reshape(count, width)
    base = feats // LANES * LANES
    tail = columns[:, base:]
    positions = lax.broadcasted_iota(jnp.int32, (1, count), 1)
    column_ids = (positions // segments * (near * wide) + me) * segments + positions % segments
    for step in range(1, near + 1):
        other = lax.rem(q + step, near)
        first = other * wide
        panel = rows[pl.ds(first, wide)].reshape(wide * segments, width)
        cosine = lax.dot_general(
            panel, columns, (((1,), (1,)), ((), ())), preferred_element_type=jnp.float32
        )
        row_ids = (z * near * wide + first) * segments + lax.broadcasted_iota(
            jnp.int32, (wide * segments, 1), 0
        )
        affinity = jnp.where(
            row_ids == column_ids, jnp.zeros_like(cosine), jnp.exp(sharpness * cosine)
        )
        sums = lax.dot_general(
            affinity.astype(jnp.bfloat16), tail, (((1,), (0,)), ((), ())),
            preferred_element_type=jnp.float32,
        )
        partial[pl.ds(first, wide)] = sums.astype(jnp.bfloat16).reshape(wide, segments, width - base)

        for dc in range(wide):
            dq = step % near
            if dq or dc:
                k = dq * wide + dc
                to = lax.rem(col + dc, wide)
                pltpu.make_async_remote_copy(
                    src_ref=partial.at[first + to],
                    dst_ref=landed.at[k],
                    send_sem=part_send.at[k],
                    recv_sem=part_recv.at[k],
                    device_id=at(z, other, to),
                    device_id_type=MESH,
                ).start()

    def part_copy(k):
        dq, dc = k // wide, k % wide
        other, to = lax.rem(q + dq, near), lax.rem(col + dc, wide)
        return pltpu.make_async_remote_copy(
            src_ref=partial.at[other * wide + to],
            dst_ref=landed.at[k],
            send_sem=part_send.at[k],
            recv_sem=part_recv.at[k],
            device_id=at(z, other, to),
            device_id_type=MESH,
        )

    total = partial[me].astype(jnp.float32)
    for k in range(1, near * wide):
        part_copy(k).wait_recv()
        total = total + landed[k].astype(jnp.float32)
    total = total.T
    low = feats - base
    out_ref[...] = total[low : low + vecs] / total[low + vecs : low + vecs + 1]

    for k in range(1, near * wide):
        part_copy(k).wait_send()
    for k in range(len(hops)):
        for piece in range(PIECES):
            if k:
                own_copy(k, piece, me, hop_to(k)).wait_send()
            pair_copy(k, piece, source(k, col)).wait_send()
    for step in range(line - 1):
        for chunk in range(CHUNKS):
            for up in (True, False):
                copy, sends = line_copy(up, step, chunk)
                pl.when(sends)(copy.wait_send)


def shards(shape, embeddings, scale_weights, vectors):
    row_count, wide = shape
    near = math.gcd(row_count, 2)
    line = row_count // near
    scales, dim, segments = embeddings.shape
    vecs = vectors.shape[0]
    feats = scales * dim
    width = -(-(feats + vecs + 1) // LANES) * LANES
    plane = near * wide
    base = feats // LANES * LANES
    hops = near * wide // CORES
    steps = max(line - 1, 1)
    dma = pltpu.SemaphoreType.DMA
    return pl.pallas_call(
        functools.partial(kernel, (line, near, wide, width)),
        out_shape=jax.ShapeDtypeStruct((vecs, segments), jnp.float32),
        in_specs=[
            pl.BlockSpec(memory_space=pl.ANY),
            pl.BlockSpec(memory_space=pltpu.SMEM),
            pl.BlockSpec(memory_space=pltpu.VMEM),
        ],
        out_specs=pl.BlockSpec(memory_space=pltpu.VMEM),
        scratch_shapes=[
            pltpu.VMEM((scales, segments, dim), jnp.bfloat16),
            dma,
            pltpu.VMEM((plane, segments, width), jnp.bfloat16),
            pltpu.VMEM((line, segments, width), jnp.bfloat16),
            pltpu.VMEM((plane, segments, width - base), jnp.bfloat16),
            pltpu.VMEM((plane, segments, width - base), jnp.bfloat16),
            dma((2, steps, CHUNKS)),
            dma((2, steps, CHUNKS)),
            dma((hops, PIECES)),
            dma((hops, PIECES)),
            dma((hops, PIECES)),
            dma((hops, PIECES)),
            dma((plane,)),
            dma((plane,)),
        ],
        compiler_params=pltpu.CompilerParams(
            collective_id=0, has_side_effects=True, vmem_limit_bytes=56 * 1024 * 1024
        ),
    )(jnp.swapaxes(embeddings, 1, 2), scale_weights, vectors)


def solution(mesh):
    placed = (P(None, None, ("row", "col")), P(), P(None, ("row", "col")))
    return jax.shard_map(
        functools.partial(shards, (mesh.shape["row"], mesh.shape["col"])),
        mesh=mesh, in_specs=placed, out_specs=P(None, ("row", "col")), check_vma=False,
    )
```

```python
import functools
import math

import jax
import jax.numpy as jnp
from jax import lax
from jax.experimental import pallas as pl
from jax.experimental.pallas import tpu as pltpu
from jax.sharding import PartitionSpec as P

SHARP = 3.5
LANES = 128
CORES = 2
CHUNKS = 4
PIECES = 2
MESH = pl.DeviceIdType.MESH


def kernel(
    plan, emb_ref, scale_ref, vec_ref, out_ref, values_ref, load_sem, rows, cols, partial, landed,
    line_send, line_recv, own_send, own_recv, pair_send, pair_recv, part_send, part_recv,
):
    line, near, wide, width = plan
    scales, segments, dim = emb_ref.shape
    vecs = vec_ref.shape[0]
    feats = scales * dim
    row, col = lax.axis_index("row"), lax.axis_index("col")
    z, q = row // near, lax.rem(row, near)
    me = q * wide + col
    partner = col + 1 - 2 * lax.rem(col, CORES)

    def at(other_z, other_q, other_col):
        return (other_z * near + other_q, other_col)

    load = pltpu.make_async_copy(emb_ref, values_ref, load_sem)
    load.start()
    barrier = pltpu.get_barrier_semaphore()
    greeted = (z > 0).astype(jnp.int32) + (z < line - 1).astype(jnp.int32)

    def greet(device):
        pl.semaphore_signal(barrier, inc=1, device_id=device, device_id_type=MESH)

    pl.when(z > 0)(lambda: greet(at(z - 1, q, col)))
    pl.when(z < line - 1)(lambda: greet(at(z + 1, q, col)))
    greet(at(z, q, partner))
    greeted = greeted + 1
    for dc in range(CORES, wide, CORES):
        greet(at(z, q, lax.rem(col + dc, wide)))
        greeted = greeted + 1
    if near > 1:
        greet(at(z, 1 - q, col))
        greeted = greeted + 1
    load.wait()

    whole = dim // LANES * LANES
    units, unit_rests, weights, weight_rests = [], [], [], []
    for s in range(scales):
        values = values_ref[s].astype(jnp.float32)
        unit = values * lax.rsqrt(jnp.sum(values * values, axis=1, keepdims=True) + 1e-06)
        unit = unit.astype(jnp.bfloat16)
        weighted = (scale_ref[s] * unit.astype(jnp.float32)).astype(jnp.bfloat16)
        units.append(unit[:, :whole])
        unit_rests.append(unit[:, whole:])
        weights.append(weighted[:, :whole])
        weight_rests.append(weighted[:, whole:])
    ones = jnp.ones((segments, width - feats - vecs), jnp.bfloat16)
    zeros = jnp.zeros((segments, width - feats), jnp.bfloat16)
    cols[z] = jnp.concatenate(units + unit_rests + [vec_ref[...].T, ones], axis=1)
    rows[me] = jnp.concatenate(weights + weight_rests + [zeros], axis=1)
    pl.semaphore_wait(barrier, greeted)

    size = segments // CHUNKS

    def line_copy(up, step, chunk):
        block = z - step if up else z + step
        there = z + 1 if up else z - 1
        piece = cols.at[jnp.clip(block, 0, line - 1), pl.ds(chunk * size, size)]
        k = int(up)
        copy = pltpu.make_async_remote_copy(
            src_ref=piece,
            dst_ref=piece,
            send_sem=line_send.at[k, step, chunk],
            recv_sem=line_recv.at[k, step, chunk],
            device_id=at(jnp.clip(there, 0, line - 1), q, col),
            device_id_type=MESH,
        )
        sends = (z - step >= 0) & (z < line - 1) if up else (z + step <= line - 1) & (z > 0)
        return copy, sends

    def line_start(up, step, chunk):
        copy, sends = line_copy(up, step, chunk)
        pl.when(sends)(copy.start)

    def line_arrive(up, step, chunk):
        block = z - 1 - step if up else z + 1 + step
        piece = cols.at[jnp.clip(block, 0, line - 1), pl.ds(chunk * size, size)]
        gets = (z - 1 - step >= 0) if up else (z + 1 + step <= line - 1)

        @pl.when(gets)
        def _():
            pltpu.make_async_remote_copy(
                src_ref=piece,
                dst_ref=piece,
                send_sem=line_send.at[int(up), step, chunk],
                recv_sem=line_recv.at[int(up), step, chunk],
                device_id=at(jnp.clip(z - 1 if up else z + 1, 0, line - 1), q, col),
                device_id_type=MESH,
            ).wait_recv()

    hops = [(dq, dc) for dq in range(near) for dc in range(0, wide, CORES)]
    pairs = wide // CORES

    part = segments // PIECES

    def own_copy(k, piece, slot, to):
        block = rows.at[slot, pl.ds(piece * part, part)]
        return pltpu.make_async_remote_copy(
            src_ref=block,
            dst_ref=block,
            send_sem=own_send.at[k, piece],
            recv_sem=own_recv.at[k, piece],
            device_id=to,
            device_id_type=MESH,
        )

    def source(k, column):
        dq, dc = hops[k]
        return lax.rem(q - dq + near, near) * wide + lax.rem(column - dc + wide, wide)

    def pair_copy(k, piece, slot):
        block = rows.at[slot, pl.ds(piece * part, part)]
        return pltpu.make_async_remote_copy(
            src_ref=block,
            dst_ref=block,
            send_sem=pair_send.at[k, piece],
            recv_sem=pair_recv.at[k, piece],
            device_id=at(z, q, partner),
            device_id_type=MESH,
        )

    def hop_to(k):
        dq, dc = hops[k]
        return at(z, 1 - q, col) if dq else at(z, q, lax.rem(col + dc, wide))

    def relay(k, piece):
        if near > 1:
            own_copy(k + pairs, piece, source(k, col), hop_to(k + pairs)).start()

    for chunk in range(CHUNKS):
        for up in (True, False):
            if line > 1:
                line_start(up, 0, chunk)
    for piece in range(PIECES):
        for k in range(1, pairs):
            own_copy(k, piece, me, hop_to(k)).start()
        relay(0, piece)
        pair_copy(0, piece, me).start()

    def plane_pass(k, piece):
        slot = source(k, col)
        own_copy(k, piece, slot, hop_to(k)).wait_recv()
        if k < pairs:
            relay(k, piece)
        pair_copy(k, piece, slot).start()

    todo = [(k, piece) for k in range(1, len(hops)) for piece in range(PIECES)]
    turns = (line - 1) * CHUNKS
    due = [1 + e * max(turns - CHUNKS + 1, 0) // max(len(todo), 1) for e in range(len(todo))]
    for turn in range(turns):
        step, chunk = turn // CHUNKS, turn % CHUNKS
        for up in (True, False):
            line_arrive(up, step, chunk)
            if step + 1 < line - 1:
                line_start(up, step + 1, chunk)
        for event, when in zip(todo, due):
            if when == turn:
                plane_pass(*event)
    for event, when in zip(todo, due):
        if when >= turns:
            plane_pass(*event)
    for k in range(len(hops)):
        for piece in range(PIECES):
            pair_copy(k, piece, source(k, partner)).wait_recv()

    sharpness = SHARP * math.sqrt(dim)
    count = line * segments
    span = width - feats
    columns = cols[...].reshape(count, width)
    base = feats // LANES * LANES
    tail = columns[:, base:]
    positions = lax.broadcasted_iota(jnp.int32, (1, count), 1)
    column_ids = (positions // segments * (near * wide) + me) * segments + positions % segments
    for step in range(1, near + 1):
        other = lax.rem(q + step, near)
        first = other * wide
        panel = rows[pl.ds(first, wide)].reshape(wide * segments, width)
        cosine = lax.dot_general(
            panel, columns, (((1,), (1,)), ((), ())), preferred_element_type=jnp.float32
        )
        row_ids = (z * near * wide + first) * segments + lax.broadcasted_iota(
            jnp.int32, (wide * segments, 1), 0
        )
        affinity = jnp.where(
            row_ids == column_ids, jnp.zeros_like(cosine), jnp.exp(sharpness * cosine)
        )
        sums = lax.dot_general(
            affinity.astype(jnp.bfloat16), tail, (((1,), (0,)), ((), ())),
            preferred_element_type=jnp.float32,
        )
        sums = sums[:, feats - base :].reshape(wide, segments, span)
        sums = jnp.concatenate([sums[:, : segments // 2], sums[:, segments // 2 :]], axis=2)
        partial[pl.ds(first, wide)] = sums.astype(jnp.bfloat16)

        for dc in reversed(range(wide)):
            dq = step % near
            if dq or dc:
                k = dq * wide + dc
                to = lax.rem(col + dc, wide)
                pltpu.make_async_remote_copy(
                    src_ref=partial.at[first + to],
                    dst_ref=landed.at[k],
                    send_sem=part_send.at[k],
                    recv_sem=part_recv.at[k],
                    device_id=at(z, other, to),
                    device_id_type=MESH,
                ).start()

    def part_copy(k):
        dq, dc = k // wide, k % wide
        other, to = lax.rem(q + dq, near), lax.rem(col + dc, wide)
        return pltpu.make_async_remote_copy(
            src_ref=partial.at[other * wide + to],
            dst_ref=landed.at[k],
            send_sem=part_send.at[k],
            recv_sem=part_recv.at[k],
            device_id=at(z, other, to),
            device_id_type=MESH,
        )

    total = partial[me].astype(jnp.float32)
    for k in range(1, near * wide):
        part_copy(k).wait_recv()
        total = total + landed[k].astype(jnp.float32)
    total = jnp.concatenate([total[:, :span], total[:, span:]], axis=0).T
    out_ref[...] = total[:vecs] / total[vecs : vecs + 1]

    for k in range(1, near * wide):
        part_copy(k).wait_send()
    for k in range(len(hops)):
        for piece in range(PIECES):
            if k:
                own_copy(k, piece, me, hop_to(k)).wait_send()
            pair_copy(k, piece, source(k, col)).wait_send()
    for step in range(line - 1):
        for chunk in range(CHUNKS):
            for up in (True, False):
                copy, sends = line_copy(up, step, chunk)
                pl.when(sends)(copy.wait_send)


def shards(shape, embeddings, scale_weights, vectors):
    row_count, wide = shape
    near = math.gcd(row_count, 2)
    line = row_count // near
    scales, dim, segments = embeddings.shape
    vecs = vectors.shape[0]
    feats = scales * dim
    width = -(-(feats + vecs + 1) // LANES) * LANES
    plane = near * wide
    hops = near * wide // CORES
    steps = max(line - 1, 1)
    dma = pltpu.SemaphoreType.DMA
    return pl.pallas_call(
        functools.partial(kernel, (line, near, wide, width)),
        out_shape=jax.ShapeDtypeStruct((vecs, segments), jnp.float32),
        in_specs=[
            pl.BlockSpec(memory_space=pl.ANY),
            pl.BlockSpec(memory_space=pltpu.SMEM),
            pl.BlockSpec(memory_space=pltpu.VMEM),
        ],
        out_specs=pl.BlockSpec(memory_space=pltpu.VMEM),
        scratch_shapes=[
            pltpu.VMEM((scales, segments, dim), jnp.bfloat16),
            dma,
            pltpu.VMEM((plane, segments, width), jnp.bfloat16),
            pltpu.VMEM((line, segments, width), jnp.bfloat16),
            pltpu.VMEM((plane, segments // 2, 2 * (width - feats)), jnp.bfloat16),
            pltpu.VMEM((plane, segments // 2, 2 * (width - feats)), jnp.bfloat16),
            dma((2, steps, CHUNKS)),
            dma((2, steps, CHUNKS)),
            dma((hops, PIECES)),
            dma((hops, PIECES)),
            dma((hops, PIECES)),
            dma((hops, PIECES)),
            dma((plane,)),
            dma((plane,)),
        ],
        compiler_params=pltpu.CompilerParams(
            collective_id=0, has_side_effects=True, vmem_limit_bytes=56 * 1024 * 1024
        ),
    )(jnp.swapaxes(embeddings, 1, 2), scale_weights, vectors)


def solution(mesh):
    placed = (P(None, None, ("row", "col")), P(), P(None, ("row", "col")))
    return jax.shard_map(
        functools.partial(shards, (mesh.shape["row"], mesh.shape["col"])),
        mesh=mesh, in_specs=placed, out_specs=P(None, ("row", "col")), check_vma=False,
    )
```

```python
import functools
import math

import jax
import jax.numpy as jnp
from jax import lax
from jax.experimental import pallas as pl
from jax.experimental.pallas import tpu as pltpu
from jax.sharding import PartitionSpec as P

SHARP = 3.5
LANES = 128
CORES = 2
CHUNKS = 4
PIECES = 2
MESH = pl.DeviceIdType.MESH


def kernel(
    plan, emb_ref, scale_ref, vec_ref, out_ref, values_ref, load_sem, rows, cols, partial, landed,
    line_send, line_recv, own_send, own_recv, pair_send, pair_recv, part_send, part_recv,
):
    line, near, wide, width = plan
    scales, segments, dim = emb_ref.shape
    vecs = vec_ref.shape[0]
    feats = scales * dim
    row, col = lax.axis_index("row"), lax.axis_index("col")
    z, q = row // near, lax.rem(row, near)
    me = q * wide + col
    partner = col + 1 - 2 * lax.rem(col, CORES)

    def at(other_z, other_q, other_col):
        return (other_z * near + other_q, other_col)

    load = pltpu.make_async_copy(emb_ref, values_ref, load_sem)
    load.start()
    barrier = pltpu.get_barrier_semaphore()
    greeted = (z > 0).astype(jnp.int32) + (z < line - 1).astype(jnp.int32)

    def greet(device):
        pl.semaphore_signal(barrier, inc=1, device_id=device, device_id_type=MESH)

    pl.when(z > 0)(lambda: greet(at(z - 1, q, col)))
    pl.when(z < line - 1)(lambda: greet(at(z + 1, q, col)))
    greet(at(z, q, partner))
    greeted = greeted + 1
    for dc in range(CORES, wide, CORES):
        greet(at(z, q, lax.rem(col + dc, wide)))
        greeted = greeted + 1
    if near > 1:
        greet(at(z, 1 - q, col))
        greeted = greeted + 1
    load.wait()

    whole = dim // LANES * LANES
    units, unit_rests, weights, weight_rests = [], [], [], []
    for s in range(scales):
        values = values_ref[s].astype(jnp.float32)
        unit = values * lax.rsqrt(jnp.sum(values * values, axis=1, keepdims=True) + 1e-06)
        unit = unit.astype(jnp.bfloat16)
        weighted = (scale_ref[s] * unit.astype(jnp.float32)).astype(jnp.bfloat16)
        units.append(unit[:, :whole])
        unit_rests.append(unit[:, whole:])
        weights.append(weighted[:, :whole])
        weight_rests.append(weighted[:, whole:])
    ones = jnp.ones((segments, width - feats - vecs), jnp.bfloat16)
    zeros = jnp.zeros((segments, width - feats), jnp.bfloat16)
    cols[z] = jnp.concatenate(units + unit_rests + [vec_ref[...].T, ones], axis=1)
    rows[me] = jnp.concatenate(weights + weight_rests + [zeros], axis=1)
    pl.semaphore_wait(barrier, greeted)

    size = segments // CHUNKS

    def line_copy(up, step, chunk):
        block = z - step if up else z + step
        there = z + 1 if up else z - 1
        piece = cols.at[jnp.clip(block, 0, line - 1), pl.ds(chunk * size, size)]
        k = int(up)
        copy = pltpu.make_async_remote_copy(
            src_ref=piece,
            dst_ref=piece,
            send_sem=line_send.at[k, step, chunk],
            recv_sem=line_recv.at[k, step, chunk],
            device_id=at(jnp.clip(there, 0, line - 1), q, col),
            device_id_type=MESH,
        )
        sends = (z - step >= 0) & (z < line - 1) if up else (z + step <= line - 1) & (z > 0)
        return copy, sends

    def line_start(up, step, chunk):
        copy, sends = line_copy(up, step, chunk)
        pl.when(sends)(copy.start)

    def line_arrive(up, step, chunk):
        block = z - 1 - step if up else z + 1 + step
        piece = cols.at[jnp.clip(block, 0, line - 1), pl.ds(chunk * size, size)]
        gets = (z - 1 - step >= 0) if up else (z + 1 + step <= line - 1)

        @pl.when(gets)
        def _():
            pltpu.make_async_remote_copy(
                src_ref=piece,
                dst_ref=piece,
                send_sem=line_send.at[int(up), step, chunk],
                recv_sem=line_recv.at[int(up), step, chunk],
                device_id=at(jnp.clip(z - 1 if up else z + 1, 0, line - 1), q, col),
                device_id_type=MESH,
            ).wait_recv()

    hops = [(dq, dc) for dq in range(near) for dc in range(0, wide, CORES)]
    pairs = wide // CORES

    part = segments // PIECES

    def own_copy(k, piece, slot, to):
        block = rows.at[slot, pl.ds(piece * part, part)]
        return pltpu.make_async_remote_copy(
            src_ref=block,
            dst_ref=block,
            send_sem=own_send.at[k, piece],
            recv_sem=own_recv.at[k, piece],
            device_id=to,
            device_id_type=MESH,
        )

    def source(k, column):
        dq, dc = hops[k]
        return lax.rem(q - dq + near, near) * wide + lax.rem(column - dc + wide, wide)

    def pair_copy(k, piece, slot):
        block = rows.at[slot, pl.ds(piece * part, part)]
        return pltpu.make_async_remote_copy(
            src_ref=block,
            dst_ref=block,
            send_sem=pair_send.at[k, piece],
            recv_sem=pair_recv.at[k, piece],
            device_id=at(z, q, partner),
            device_id_type=MESH,
        )

    def hop_to(k):
        dq, dc = hops[k]
        return at(z, 1 - q, col) if dq else at(z, q, lax.rem(col + dc, wide))

    def relay(k, piece):
        if near > 1:
            own_copy(k + pairs, piece, source(k, col), hop_to(k + pairs)).start()

    for chunk in range(CHUNKS):
        for up in (True, False):
            if line > 1:
                line_start(up, 0, chunk)
    for piece in range(PIECES):
        for k in range(1, pairs):
            own_copy(k, piece, me, hop_to(k)).start()
        relay(0, piece)
        pair_copy(0, piece, me).start()

    def plane_pass(k, piece):
        slot = source(k, col)
        own_copy(k, piece, slot, hop_to(k)).wait_recv()
        if k < pairs:
            relay(k, piece)
        pair_copy(k, piece, slot).start()

    todo = [(k, piece) for k in range(1, len(hops)) for piece in range(PIECES)]
    turns = (line - 1) * CHUNKS
    due = [1 + e * max(turns - CHUNKS + 1, 0) // max(len(todo), 1) for e in range(len(todo))]
    for turn in range(turns):
        step, chunk = turn // CHUNKS, turn % CHUNKS
        for up in (True, False):
            line_arrive(up, step, chunk)
            if step + 1 < line - 1:
                line_start(up, step + 1, chunk)
        for event, when in zip(todo, due):
            if when == turn:
                plane_pass(*event)
    for event, when in zip(todo, due):
        if when >= turns:
            plane_pass(*event)
    for k in range(len(hops)):
        for piece in range(PIECES):
            pair_copy(k, piece, source(k, partner)).wait_recv()

    sharpness = SHARP * math.sqrt(dim)
    count = line * segments
    columns = cols[...].reshape(count, width)
    base = feats // LANES * LANES
    tail = columns[:, base:]
    positions = lax.broadcasted_iota(jnp.int32, (1, count), 1)
    column_ids = (positions // segments * (near * wide) + me) * segments + positions % segments
    for step in range(1, near + 1):
        other = lax.rem(q + step, near)
        first = other * wide
        panel = rows[pl.ds(first, wide)].reshape(wide * segments, width)
        cosine = lax.dot_general(
            panel, columns, (((1,), (1,)), ((), ())), preferred_element_type=jnp.float32
        )
        row_ids = (z * near * wide + first) * segments + lax.broadcasted_iota(
            jnp.int32, (wide * segments, 1), 0
        )
        affinity = jnp.where(
            row_ids == column_ids, jnp.zeros_like(cosine), jnp.exp(sharpness * cosine)
        )
        sums = lax.dot_general(
            affinity.astype(jnp.bfloat16), tail, (((1,), (0,)), ((), ())),
            preferred_element_type=jnp.float32,
        )
        partial[pl.ds(first, wide)] = sums.astype(jnp.bfloat16).reshape(wide, segments, width - base)

        for dc in range(wide):
            dq = step % near
            if dq or dc:
                k = dq * wide + dc
                to = lax.rem(col + dc, wide)
                pltpu.make_async_remote_copy(
                    src_ref=partial.at[first + to],
                    dst_ref=landed.at[k],
                    send_sem=part_send.at[k],
                    recv_sem=part_recv.at[k],
                    device_id=at(z, other, to),
                    device_id_type=MESH,
                ).start()

    def part_copy(k):
        dq, dc = k // wide, k % wide
        other, to = lax.rem(q + dq, near), lax.rem(col + dc, wide)
        return pltpu.make_async_remote_copy(
            src_ref=partial.at[other * wide + to],
            dst_ref=landed.at[k],
            send_sem=part_send.at[k],
            recv_sem=part_recv.at[k],
            device_id=at(z, other, to),
            device_id_type=MESH,
        )

    total = partial[me].astype(jnp.float32)
    for k in range(1, near * wide):
        part_copy(k).wait_recv()
        total = total + landed[k].astype(jnp.float32)
    total = total.T
    low = feats - base
    out_ref[...] = total[low : low + out_ref.shape[0]]

    for k in range(1, near * wide):
        part_copy(k).wait_send()
    for k in range(len(hops)):
        for piece in range(PIECES):
            if k:
                own_copy(k, piece, me, hop_to(k)).wait_send()
            pair_copy(k, piece, source(k, col)).wait_send()
    for step in range(line - 1):
        for chunk in range(CHUNKS):
            for up in (True, False):
                copy, sends = line_copy(up, step, chunk)
                pl.when(sends)(copy.wait_send)


def shards(shape, embeddings, scale_weights, vectors):
    row_count, wide = shape
    near = math.gcd(row_count, 2)
    line = row_count // near
    scales, dim, segments = embeddings.shape
    vecs = vectors.shape[0]
    feats = scales * dim
    width = -(-(feats + vecs + 1) // LANES) * LANES
    plane = near * wide
    base = feats // LANES * LANES
    hops = near * wide // CORES
    steps = max(line - 1, 1)
    dma = pltpu.SemaphoreType.DMA
    sums = pl.pallas_call(
        functools.partial(kernel, (line, near, wide, width)),
        out_shape=jax.ShapeDtypeStruct((width - feats, segments), jnp.float32),
        in_specs=[
            pl.BlockSpec(memory_space=pl.ANY),
            pl.BlockSpec(memory_space=pltpu.SMEM),
            pl.BlockSpec(memory_space=pltpu.VMEM),
        ],
        out_specs=pl.BlockSpec(memory_space=pltpu.VMEM),
        scratch_shapes=[
            pltpu.VMEM((scales, segments, dim), jnp.bfloat16),
            dma,
            pltpu.VMEM((plane, segments, width), jnp.bfloat16),
            pltpu.VMEM((line, segments, width), jnp.bfloat16),
            pltpu.VMEM((plane, segments, width - base), jnp.bfloat16),
            pltpu.VMEM((plane, segments, width - base), jnp.bfloat16),
            dma((2, steps, CHUNKS)),
            dma((2, steps, CHUNKS)),
            dma((hops, PIECES)),
            dma((hops, PIECES)),
            dma((hops, PIECES)),
            dma((hops, PIECES)),
            dma((plane,)),
            dma((plane,)),
        ],
        compiler_params=pltpu.CompilerParams(
            collective_id=0, has_side_effects=True, vmem_limit_bytes=56 * 1024 * 1024
        ),
    )(jnp.swapaxes(embeddings, 1, 2), scale_weights, vectors)
    return sums[:vecs] / sums[vecs : vecs + 1]


def solution(mesh):
    placed = (P(None, None, ("row", "col")), P(), P(None, ("row", "col")))
    return jax.shard_map(
        functools.partial(shards, (mesh.shape["row"], mesh.shape["col"])),
        mesh=mesh, in_specs=placed, out_specs=P(None, ("row", "col")), check_vma=False,
    )
```
